32 devices in a mesh: seq: 8 (over z, y), ch: 4 (over x, core).
Axes of the slice: x: 2, y: 2, z: 4, core: 2. Of those that a mesh axis runs over, the one named last changes fastest.
Arguments:
- inputs: bfloat16 [8192, 768], P(('seq', 'ch')), may hold values from -6 to 6
- gain_one: float32 [768], replicated, may hold values from 0.5 to 1.5
- shift_one: float32 [768], replicated, may hold values from -1.5 to 1.5
- conv_weight: bfloat16 [3, 768, 384], P(None, None, 'ch'), may hold values from -0.125 to 0.125
- gain_two: float32 [384], P('ch'), may hold values from 0.5 to 1.5
- shift_two: float32 [384], P('ch'), may hold values from -1.5 to 1.5
- mix_weight: bfloat16 [384, 768], P('ch'), may hold values from -0.3125 to 0.3125
- head_weight: bfloat16 [768, 6956], P('ch'), may hold values from -0.21875 to 0.21875
- head_bias: float32 [6956], replicated, may hold values from -2 to 2
- species: int32 [8], replicated, may hold values from 0 to 1, as said below
- counts: int32 [8192, 5313], P(('seq', 'ch')), may hold values from 0 to 3
Outputs:
- outputs: bfloat16 [8192, 768], P(('seq', 'ch'))
- input_grad: float32 [8192, 768], P(('seq', 'ch'))
- gain_one_grad: float32 [768], replicated
- shift_one_grad: float32 [768], replicated
- conv_weight_grad: float32 [3, 768, 384], P(None, None, 'ch')
- gain_two_grad: float32 [384], P('ch')
- shift_two_grad: float32 [384], P('ch')
- mix_weight_grad: float32 [384, 768], P('ch')
- head_weight_grad: float32 [768, 6956], P(('seq', 'ch'))
- head_bias_grad: float32 [6956], replicated
The draws below stay inside these ranges and needn't reach their ends.
Inputs may be any that keep to these rules, and one draw needn't show every extreme that they name: Each window holds one species, given by species[w]; both species occur in every draw.
All inputs are finite; a program needn't handle non-finite values.
Results may differ from the reference program's by a relative error of at most 0.014.
Values may be sent and summed in bfloat16 or wider, within the bound.
A program may use at most 192 MiB of HBM per device.

```python
import jax
import jax.numpy as jnp
from jax import lax

D = 768
H = 384
HUMAN = 5313
MOUSE = 1643
DILATION_STEP = 11
TAPS = 3
WINDOW_BINS = 1024
SHIFT = 512
BINS = 8192
NWIN = 8
TRACKS = 6956


def draw_species(key, part):
    order = jax.random.permutation(key, NWIN)
    return (jnp.mod(order, 3) == 0).astype(jnp.int32)


def plant(entries, stream_key, least, largest):
    index_at = [jax.random.randint(jax.random.fold_in(stream_key, axis), (), 0, length) for axis, length in enumerate(entries.shape)]
    main_axis = entries.shape.index(max(entries.shape))
    neighbour = index_at[:main_axis] + [(index_at[main_axis] + 1) % entries.shape[main_axis]] + index_at[main_axis + 1:]
    return entries.at[tuple(index_at)].set(least).at[tuple(neighbour)].set(largest)


def raised(array, own_key, source, target, shards_of, factor):
    def block_of(axis_at):
        return (jnp.arange(array.shape[axis_at]) // (array.shape[axis_at] // shards_of)).reshape((-1,) + (1,) * (array.ndim - 1 - axis_at))

    first = jax.random.permutation(own_key, shards_of)[block_of(target)]
    second = (block_of(target) + shards_of // 2) % shards_of
    return jnp.where((block_of(source) == first) | (block_of(source) == second), factor * array, array)


def steps_of(own_key, shape, pieces, low, largest):
    loudness = 1.0
    for axis_at, shards_of in pieces:
        heights = jax.random.uniform(jax.random.fold_in(jax.random.fold_in(own_key, 6), axis_at), (shards_of,), jnp.float32, low / len(pieces), largest / len(pieces))
        loudness = loudness * jnp.repeat(jnp.exp(heights), shape[axis_at] // shards_of).reshape((-1,) + (1,) * (len(shape) - 1 - axis_at))
    return loudness


def noise(own_key, shape, scale, reach, split=(), dtype=jnp.bfloat16):
    values = jax.random.normal(own_key, shape, jnp.float32) * scale
    if len(split) > 0:
        values = steps_of(own_key, shape, split, -0.22, 0.18) * values
    return jnp.clip(values, min=-reach, max=reach).astype(dtype)


def bell_draw_with(rng, extent, scale, bound, split, heavy, held_as=jnp.bfloat16):
    result = scale * jax.random.normal(rng, extent, jnp.float32)
    if split:
        result = result * steps_of(rng, extent, split, -0.22, 0.18)
    return jnp.clip(raised(result, jax.random.fold_in(rng, 3), *heavy), -bound, bound).astype(held_as)


def setup_inputs(seed: int = 0) -> dict:
    key_of = jax.random.split(jax.random.key(seed), 12)
    inputs = bell_draw_with(key_of[0], (BINS, D), 1.0, 6.0, ((0, 32),), (0, 1, 32, 2.75))
    gain_one = jnp.clip(1.0 + 0.1 * jax.random.normal(key_of[1], (D,), jnp.float32), 0.5, 1.5)
    shift_one = noise(key_of[2], (D,), 0.3, 1.5, (), jnp.float32)
    conv_weight = noise(key_of[3], (TAPS, D, H), (TAPS * D) ** -0.5, 0.125, ((2, 4),))
    gain_two = jnp.clip(1.0 + 0.1 * jax.random.normal(key_of[4], (H,), jnp.float32), 0.5, 1.5)
    shift_two = noise(key_of[5], (H,), 0.3, 1.5, ((0, 4),), jnp.float32)
    mix_weight = noise(key_of[6], (H, D), H ** -0.5, 0.3125, ((0, 4),))
    head_weight = noise(key_of[7], (D, TRACKS), D ** -0.5, 0.21875, ((0, 4),))
    head_bias = noise(key_of[8], (TRACKS,), 0.5, 2.0, (), jnp.float32)
    species = draw_species(jax.random.fold_in(key_of[11], 71), 0)
    counts = plant(jax.random.randint(key_of[10], (BINS, HUMAN), 0, 4), jax.random.fold_in(key_of[10], 1), 0, 3).astype(jnp.int32)
    return {"inputs": inputs, "gain_one": gain_one, "shift_one": shift_one, "conv_weight": conv_weight, "gain_two": gain_two, "shift_two": shift_two, "mix_weight": mix_weight, "head_weight": head_weight, "head_bias": head_bias, "species": species, "counts": counts}


norm_eps = 1e-05
highest = lax.Precision.HIGHEST

@jax.custom_vjp
def low(v):
    return lax.optimization_barrier(v.astype(jnp.bfloat16)).astype(jnp.float32)

@jax.custom_vjp
def low_back(v):
    return v

def low_keep(v):
    return (low(v), None)

def low_pass(kept, grad):
    return (grad,)

def back_keep(v):
    return (v, None)

def back_low(kept, grad):
    return (low(grad),)
low.defvjp(low_keep, low_pass)
low_back.defvjp(back_keep, back_low)

def batch_norm(values, gain, offset):
    center = lax.optimization_barrier(jnp.mean(values, 0))
    deviation = values - center
    spread = lax.optimization_barrier(jnp.mean(deviation * deviation, 0))
    return deviation * lax.rsqrt(spread + norm_eps) * gain + offset

def poisson_sum(logits, target):
    rate = jax.nn.softplus(logits)
    return jnp.sum(rate - target * jnp.log(rate))

def reference(inputs, gain_one, shift_one, conv_weight, gain_two, shift_two, mix_weight, head_weight, head_bias, species, counts):
    targets = jnp.roll(counts.astype(jnp.float32), -SHIFT, 0).reshape(NWIN, WINDOW_BINS, HUMAN)

    def forward(input_f, gain_a, shift_a, conv_f, gain_b, shift_b, mix_f, head_f, bias_f):
        act_one = low(jax.nn.gelu(batch_norm(input_f, gain_a, shift_a)))
        window_list = jnp.roll(act_one, -SHIFT, 0).reshape(NWIN, WINDOW_BINS, D)
        padded_input = jnp.pad(window_list, ((0, 0), (DILATION_STEP, DILATION_STEP), (0, 0)))
        conv_sum = jnp.zeros((NWIN, WINDOW_BINS, H), jnp.float32)
        for kernel_tap_index in range(TAPS):
            part = padded_input[:, kernel_tap_index * DILATION_STEP:kernel_tap_index * DILATION_STEP + WINDOW_BINS]
            conv_sum = conv_sum + jnp.einsum('nwi,ij->nwj', part, conv_f[kernel_tap_index], precision=highest)
        conv_out = low_back(jnp.roll(conv_sum.reshape(BINS, H), SHIFT, 0))
        act_two = low(jax.nn.gelu(batch_norm(conv_out, gain_b, shift_b)))
        branch = low_back(jnp.dot(act_two, mix_f, precision=highest, preferred_element_type=jnp.float32))
        outputs = low(input_f + branch)
        feats = jnp.roll(outputs, -SHIFT, 0).reshape(NWIN, WINDOW_BINS, D)

        def window_loss(total, item):
            feat, target, kind = item

            def human_loss(unused):
                logits = low_back(jnp.dot(feat, head_f[:, :HUMAN], precision=highest, preferred_element_type=jnp.float32) + bias_f[:HUMAN])
                return poisson_sum(logits, target)

            def mouse_loss(unused):
                logits = low_back(jnp.dot(feat, head_f[:, HUMAN:], precision=highest, preferred_element_type=jnp.float32) + bias_f[HUMAN:])
                return poisson_sum(logits, target[:, :MOUSE])
            return (total + lax.cond(kind == 0, human_loss, mouse_loss, 0), None)
        loss, _ = lax.scan(jax.checkpoint(window_loss), jnp.zeros((), jnp.float32), (feats, targets, species))
        return (loss, outputs)
    primals = (inputs.astype(jnp.float32), gain_one, shift_one, conv_weight.astype(jnp.float32), gain_two, shift_two, mix_weight.astype(jnp.float32), head_weight.astype(jnp.float32), head_bias)
    loss, pullback, outputs = jax.vjp(forward, *primals, has_aux=True)
    grads = pullback(jnp.ones((), jnp.float32))
    return (outputs.astype(jnp.bfloat16), grads[0], grads[1], grads[2], grads[3], grads[4], grads[5], grads[6], grads[7], grads[8])
```

```python
import jax
import jax.numpy as jnp
from jax import lax
from jax.experimental import pallas as pl
from jax.experimental.pallas import tpu as pltpu
from jax.sharding import PartitionSpec as P

HUMAN = 5313
MOUSE = 1643
DILATION_STEP = 11
TAPS = 3
WINDOW_BINS = 1024
SHIFT = 512


norm_eps = 1e-05
contract_rows = (((0,), (0,)), ((), ()))
contract_cols = (((1,), (1,)), ((), ()))


def with_halo(cells, sides, width):
    for axis, dim in sides:
        count = lax.axis_size(axis)
        head = lax.slice_in_dim(cells, 0, width, axis=dim)
        tail = lax.slice_in_dim(cells, cells.shape[dim] - width, cells.shape[dim], axis=dim)
        cells = jnp.concatenate(
            [
                lax.ppermute(tail, axis, [(i, (i + 1) % count) for i in range(count)]),
                cells,
                lax.ppermute(head, axis, [((i + 1) % count, i) for i in range(count)]),
            ],
            axis=dim,
        )
    return cells


def window_lookup(position, total_bins):
    return jnp.mod(position - SHIFT, total_bins) // WINDOW_BINS


def gelu_grad(value, upstream):
    _, pullback = jax.vjp(jax.nn.gelu, value)
    return pullback(upstream)[0]


def poisson_grad(logits, target):
    rate = jax.nn.softplus(logits)
    return (jax.nn.sigmoid(logits) * (1.0 - target / rate)).astype(jnp.bfloat16)


def on_device(
    inputs,
    gain_one,
    shift_one,
    conv_weight,
    gain_two,
    shift_two,
    mix_weight,
    head_weight,
    head_bias,
    species,
    counts,
):
    seq_count = lax.axis_size("seq")
    ch_count = lax.axis_size("ch")
    seq_index = lax.axis_index("seq")
    ch_index = lax.axis_index("ch")
    local_rows = inputs.shape[0]
    width = inputs.shape[1]
    conv_cols = conv_weight.shape[2]
    residual_rows = local_rows * ch_count
    every_bin_list = residual_rows * seq_count
    inv_bins = 1.0 / every_bin_list
    input_f = inputs.astype(jnp.float32)
    sum_one, square_one = lax.psum(
        (jnp.sum(input_f, 0), jnp.sum(input_f * input_f, 0)), ("seq", "ch")
    )
    mean_one = sum_one * inv_bins
    scale_one = lax.rsqrt(square_one * inv_bins - mean_one * mean_one + norm_eps)
    normed_one = (input_f - mean_one) * scale_one
    pre_one = normed_one * gain_one + shift_one
    act_one = jax.nn.gelu(pre_one).astype(jnp.bfloat16)
    residual_block = lax.all_gather(act_one, "ch", axis=0, tiled=True)
    padded_input = with_halo(residual_block, (("seq", 0),), DILATION_STEP)
    bin_positions = seq_index * residual_rows + jnp.arange(residual_rows, dtype=jnp.int32)
    local_window = window_lookup(bin_positions, every_bin_list)
    fwd_masks = [
        window_lookup(bin_positions + (kernel_tap_index - 1) * DILATION_STEP, every_bin_list)
        == local_window
        for kernel_tap_index in range(TAPS)
    ]
    back_masks = [
        (
            window_lookup(bin_positions - (kernel_tap_index - 1) * DILATION_STEP, every_bin_list)
            == local_window
        ).astype(jnp.float32)[:, None]
        for kernel_tap_index in range(TAPS)
    ]
    conv_out = jnp.zeros((residual_rows, conv_cols), jnp.float32)
    for kernel_tap_index in range(TAPS):
        product = jnp.dot(
            padded_input[
                kernel_tap_index * DILATION_STEP : kernel_tap_index * DILATION_STEP + residual_rows
            ],
            conv_weight[kernel_tap_index],
            preferred_element_type=jnp.float32,
        )
        conv_out = conv_out + jnp.where(fwd_masks[kernel_tap_index][:, None], product, 0.0)
    sum_two, square_two = lax.psum((jnp.sum(conv_out, 0), jnp.sum(conv_out * conv_out, 0)), "seq")
    mean_two = sum_two * inv_bins
    scale_two = lax.rsqrt(square_two * inv_bins - mean_two * mean_two + norm_eps)
    normed_two = (conv_out - mean_two) * scale_two
    pre_two = normed_two * gain_two + shift_two
    act_two = jax.nn.gelu(pre_two).astype(jnp.bfloat16)
    branch = lax.psum_scatter(
        jnp.dot(act_two, mix_weight, preferred_element_type=jnp.float32).astype(jnp.bfloat16),
        "ch",
        scatter_dimension=0,
        tiled=True,
    ).astype(jnp.float32)
    outputs = (input_f + branch).astype(jnp.bfloat16)
    row_start = seq_index * residual_rows + ch_index * local_rows
    window_index = window_lookup(row_start, every_bin_list)
    window_ids = jnp.arange(species.shape[0], dtype=jnp.int32)
    my_species = jnp.sum(jnp.where(window_ids == window_index, species, 0))
    is_human = my_species == 0
    targets = counts.astype(jnp.float32)
    zero_human = jnp.zeros((local_rows, HUMAN), jnp.bfloat16)
    zero_mouse = jnp.zeros((local_rows, MOUSE), jnp.bfloat16)
    start_logits = (
        jnp.zeros((local_rows, HUMAN), jnp.float32),
        jnp.zeros((local_rows, MOUSE), jnp.float32),
    )
    piece = lax.all_gather(head_weight, "ch", axis=0, tiled=True)

    def human_add(unused):
        return (
            jnp.dot(outputs, piece[:, :HUMAN], preferred_element_type=jnp.float32),
            start_logits[1],
        )

    def mouse_add(unused):
        return (
            start_logits[0],
            jnp.dot(outputs, piece[:, HUMAN:], preferred_element_type=jnp.float32),
        )

    logit_sums = lax.cond(is_human, human_add, mouse_add, 0)

    def human_grads(unused):
        return (poisson_grad(logit_sums[0] + head_bias[:HUMAN], targets), zero_mouse)

    def mouse_grads(unused):
        return (zero_human, poisson_grad(logit_sums[1] + head_bias[HUMAN:], targets[:, :MOUSE]))

    grad_human, grad_mouse = lax.cond(is_human, human_grads, mouse_grads, 0)

    def back_piece(piece):

        def human_back(unused):
            return lax.dot_general(
                grad_human, piece[:, :HUMAN], contract_cols, preferred_element_type=jnp.float32
            )

        def mouse_back(unused):
            return lax.dot_general(
                grad_mouse, piece[:, HUMAN:], contract_cols, preferred_element_type=jnp.float32
            )

        return lax.cond(is_human, human_back, mouse_back, 0)

    grad_out = back_piece(lax.all_gather(head_weight, "ch", axis=0, tiled=True))

    def human_term(unused):
        part = lax.dot_general(
            outputs, grad_human, contract_rows, preferred_element_type=jnp.float32
        )
        return jnp.concatenate(
            [
                part,
                jnp.zeros(
                    (lax.axis_size(("seq", "ch")) * (width // (seq_count * ch_count)), MOUSE),
                    jnp.float32,
                ),
            ],
            1,
        )

    def mouse_term(unused):
        part = lax.dot_general(
            outputs, grad_mouse, contract_rows, preferred_element_type=jnp.float32
        )
        return jnp.concatenate(
            [
                jnp.zeros(
                    (lax.axis_size(("seq", "ch")) * (width // (seq_count * ch_count)), HUMAN),
                    jnp.float32,
                ),
                part,
            ],
            1,
        )

    head_weight_grad = lax.psum_scatter(
        lax.cond(is_human, human_term, mouse_term, 0),
        ("seq", "ch"),
        scatter_dimension=0,
        tiled=True,
    )
    bias_part = jnp.concatenate(
        [jnp.sum(grad_human.astype(jnp.float32), 0), jnp.sum(grad_mouse.astype(jnp.float32), 0)]
    )
    grad_branch = grad_out.astype(jnp.bfloat16)
    mix_piece = lax.all_gather(grad_branch, "ch", axis=0, tiled=True)
    grad_rows = lax.dot_general(
        mix_piece, mix_weight, contract_cols, preferred_element_type=jnp.float32
    )
    grad_acts = grad_rows
    mix_part = lax.dot_general(
        act_two, mix_piece, contract_rows, preferred_element_type=jnp.float32
    )
    grad_pre_two = gelu_grad(pre_two, grad_acts)
    gain_part = jnp.sum(grad_pre_two * normed_two, 0)
    shift_part = jnp.sum(grad_pre_two, 0)
    gain_two_grad, shift_two_grad = lax.psum((gain_part, shift_part), "seq")
    convolution_gradient = (
        gain_two
        * scale_two
        * (grad_pre_two - shift_two_grad * inv_bins - normed_two * gain_two_grad * inv_bins)
    ).astype(jnp.bfloat16)
    padded_gradient = with_halo(convolution_gradient, (("seq", 0),), DILATION_STEP)
    conv_part = jnp.stack(
        [
            lax.dot_general(
                padded_input[
                    kernel_tap_index * DILATION_STEP : kernel_tap_index * DILATION_STEP
                    + residual_rows
                ],
                jnp.where(
                    fwd_masks[kernel_tap_index][:, None],
                    convolution_gradient,
                    jnp.zeros_like(convolution_gradient),
                ),
                contract_rows,
                preferred_element_type=jnp.float32,
            )
            for kernel_tap_index in range(TAPS)
        ]
    )
    total = jnp.zeros((lax.axis_size("ch") * local_rows, width), jnp.float32)
    for kernel_tap_index in range(TAPS):
        grad_rows = lax.dynamic_slice_in_dim(
            padded_gradient,
            (2 - kernel_tap_index) * DILATION_STEP,
            lax.axis_size("ch") * local_rows,
            0,
        )
        product = lax.dot_general(
            grad_rows,
            conv_weight[kernel_tap_index],
            contract_cols,
            preferred_element_type=jnp.float32,
        )
        total = total + product * back_masks[kernel_tap_index]
    grad_act_one = lax.psum_scatter(
        total.astype(jnp.bfloat16), "ch", scatter_dimension=0, tiled=True
    ).astype(jnp.float32)
    grad_pre_one = gelu_grad(pre_one, grad_act_one)
    gain_one_grad, shift_one_grad, head_bias_grad = lax.psum(
        (jnp.sum(grad_pre_one * normed_one, 0), jnp.sum(grad_pre_one, 0), bias_part), ("seq", "ch")
    )
    input_grad = grad_out + gain_one * scale_one * (
        grad_pre_one - shift_one_grad * inv_bins - normed_one * gain_one_grad * inv_bins
    )
    conv_weight_grad, mix_weight_grad = lax.psum((conv_part, mix_part), "seq")
    return (
        outputs,
        input_grad,
        gain_one_grad,
        shift_one_grad,
        conv_weight_grad,
        gain_two_grad,
        shift_two_grad,
        mix_weight_grad,
        head_weight_grad,
        head_bias_grad,
    )


F32 = jnp.float32
BF16 = jnp.bfloat16
TILE = 384
MESH_ID = pl.DeviceIdType.MESH
GELU_C = 0.7978845608028654
GELU_A = 0.044715


def gelu_of(v):
    return 0.5 * v * (1.0 + jnp.tanh(GELU_C * (v + GELU_A * v * v * v)))


def gelu_slope(v):
    t = jnp.tanh(GELU_C * (v + GELU_A * v * v * v))
    return 0.5 * (1.0 + t) + 0.5 * v * (1.0 - t * t) * (GELU_C * (1.0 + 3.0 * GELU_A * v * v))


def logit_slope(z, n):
    e = jnp.exp(-jnp.abs(z))
    u = 1.0 + e
    log_u = jnp.log(u)
    small = e < 0.01
    series = 1.0 - e * (0.5 - e * (1.0 / 3.0 - e * (0.25 - 0.2 * e)))
    plus = z >= 0.0
    tail = jnp.where(small, series, log_u)
    rate = jnp.where(plus, z + jnp.where(small, e * series, log_u), tail)
    top = jnp.where(plus, 1.0, e)
    num = jnp.where(small, 1.0, top)
    return (top * rate - n * num) / (u * rate)


def tree(parts):
    while len(parts) > 1:
        parts = [parts[i] + parts[i + 1] for i in range(0, len(parts), 2)]
    return parts[0]


def dot_nn(a, b):
    return jnp.dot(a, b, preferred_element_type=F32)


def dot_nt(a, b):
    return lax.dot_general(a, b, (((1,), (1,)), ((), ())), preferred_element_type=F32)


def flip(i, unit):
    return i + unit - 2 * unit * ((i // unit) % 2)


def step_kernel(
    x_ref, p1_ref, g2_ref, cwo_ref, w_ref, wm_ref, cs_ref, bv_ref, flag_ref,
    out_ref, ig_ref, s1_ref, s2_ref, cg_ref, oh_ref, om_ref, bg_ref,
    act, hin, cw, conv, tap0, tap2, wh, wm, wsel, cnt, orow, ocol, gs, gacc, grecv,
    pbuf, r1, b1, r2, b2, r3, b3, r4, fin, frecv,
    m1, m2, m3, m4, a1, a2, a3, a4, z1, z2, z3, z4, q1, q2, q3, q4,
    bl, bxy, bs, bz, gpad, gsend, ghalo, gk, act2, cgb, crc, csc, crx, csx, cry, csy, crz, csz, crw, cao,
    st_s, st_r, hs_s, hs_r, cw_s, cw_r, wl_s, ws_s, ws_r, wx_s, wx_r, wy_s, wy_r, ct_l, ct_s, ct_r,
    ox_s, ox_r, rs_s, rs_r, fx_s, fx_r, bx_s, bx_r, gh_s, gh_r, cg_s, cg_r,
):
    seq = lax.axis_index("seq")
    ch = lax.axis_index("ch")
    nseq = lax.axis_size("seq")
    rows = x_ref.shape[0]
    k = ch % 2
    xb = ch // 2
    yb = seq % 2
    z0 = (seq // 2) % 2
    z1b = (seq // 4) % 2
    inv = 1.0 / (rows * nseq * 4)
    sib = (seq, ch + 1 - 2 * k)
    xpeer = (seq, flip(ch, 2))
    ypeer = (flip(seq, 1), ch)
    zpeers = ((flip(seq, 2), ch), (flip(seq, 4), ch), (flip(flip(seq, 2), 4), ch))
    near = []
    for r in range(1, 8):
        c = flip(ch, 1) if r % 2 else ch
        c = flip(c, 2) if (r // 2) % 2 else c
        near.append((flip(seq, 1) if r // 4 else seq, c))
    line = seq * 4 + ch
    after = (line + 1) % (nseq * 4)
    before = (line + nseq * 4 - 1) % (nseq * 4)
    after_id = (after // 4, after % 4)
    before_id = (before // 4, before % 4)

    def rcopy(src, dst, ss, rs, who):
        return pltpu.make_async_remote_copy(
            src_ref=src, dst_ref=dst, send_sem=ss, recv_sem=rs, device_id=who, device_id_type=MESH_ID
        )

    sent = []

    def go(copy):
        copy.start()
        sent.append(copy)
        return copy

    barrier = pltpu.get_barrier_semaphore()
    for who in [*near, *zpeers, after_id, before_id]:
        pl.semaphore_signal(barrier, inc=1, device_id=who, device_id_type=MESH_ID)

    def small_start(i, msg, slots):
        return [go(rcopy(msg, slots.at[r], st_s.at[i, r], st_r.at[i, r], near[r])) for r in range(7)]

    def small_mid(i, copies, msg, slots, mid, zslots):
        for c in copies:
            c.wait_recv()
        mid[...] = tree([msg[...]] + [slots[r] for r in range(7)])
        return [go(rcopy(mid, zslots.at[r], st_s.at[i, 7 + r], st_r.at[i, 7 + r], zpeers[r])) for r in range(3)]

    def small_end(copies, mid, zslots):
        for c in copies:
            c.wait_recv()
        return tree([mid[...]] + [zslots[r] for r in range(3)])

    own_rows = pl.ds(pl.multiple_of(192 * ch, 192), 192)

    def human_cols(j, half):
        return pl.ds(pl.multiple_of(2688 * half + TILE * j, 128), TILE)

    def mouse_cols(j, half):
        return pl.ds(pl.multiple_of(896 * half + TILE * j, 128), TILE if j < 2 else 128)

    def w_src(t, half):
        return w_ref.at[:, human_cols(t, half)] if t < 7 else wm_ref.at[:, mouse_cols(t - 7, half)]

    def w_dst(t, block):
        rows_at = pl.ds(pl.multiple_of(192 * block, 192), 192)
        if t < 7:
            return wh.at[t, rows_at, :]
        return wm.at[t - 7, rows_at, :] if t < 9 else wm.at[2, rows_at, pl.ds(0, 128)]

    order = (0, 7, 1, 8, 2, 9, 3, 4, 5, 6)
    wm[2, :, 128:] = jnp.zeros((768, TILE - 128), BF16)
    local = []
    for t in order:
        c = pltpu.make_async_copy(w_src(t, k), w_dst(t, ch), wl_s.at[t])
        c.start()
        local.append(c)
    my_bins = pl.ds(pl.multiple_of(rows * k, rows), rows)
    for j in range(7):
        c = pltpu.make_async_copy(cs_ref.at[k, :, pl.ds(TILE * j, TILE)], cnt.at[j, my_bins, :], ct_l.at[j])
        c.start()
        local.append(c)
    own_cw = pl.ds(pl.multiple_of(96 * ch, 96), 96)
    c = pltpu.make_async_copy(cwo_ref, cw.at[own_cw, :], cw_s.at[5])
    c.start()
    local.append(c)
    xf = x_ref[...].astype(F32)
    xs = jnp.sum(xf, 0, keepdims=True)
    xq = jnp.sum(xf * xf, 0, keepdims=True)
    m1[0:1, :] = xs[:, :TILE]
    m1[1:2, :] = xs[:, TILE:]
    m1[2:3, :] = xq[:, :TILE]
    m1[3:4, :] = xq[:, TILE:]
    m1[4:6, :] = g2_ref[...]
    m1[6:8, :] = jnp.zeros((2, TILE), F32)
    pl.semaphore_wait(barrier, 12)

    e1 = small_start(0, m1, a1)
    cw_sib = go(rcopy(cwo_ref, cw.at[own_cw, :], cw_s.at[0], cw_r.at[0], sib))

    def half_rows(c, h):
        return pl.ds(pl.multiple_of(96 * c + 48 * h, 48), 48)

    cw_x = go(rcopy(cwo_ref.at[pl.ds(pl.multiple_of(48 * yb, 48), 48), :], cw.at[half_rows(ch, yb), :], cw_s.at[1], cw_r.at[1], xpeer))
    xch = flip(ch, 2)
    wx = {}

    def send_w(t):
        who = (seq, flip(ch, 2) + yb * (1 - 2 * k))
        half = k + yb * (1 - 2 * k)
        wx[t] = go(rcopy(w_src(t, half), w_dst(t, ch), wx_s.at[t], wx_r.at[t], who))

    wsib = {}

    def send_w_sib(t):
        wsib[t] = go(rcopy(w_src(t, 1 - k), w_dst(t, ch), ws_s.at[t], ws_r.at[t], sib))

    wy = {}

    def pass_w(t):
        wx[t].wait_recv()
        block = xch + yb * (1 - 2 * k)
        wy[t] = go(rcopy(w_dst(t, block), w_dst(t, block), wy_s.at[t], wy_r.at[t], ypeer))

    for t in order[:2]:
        send_w_sib(t)
    e1 = small_mid(0, e1, m1, a1, q1, z1)
    send_w(order[0])
    cw_x.wait_recv()
    cw_y = go(rcopy(cw.at[half_rows(xch, yb), :], cw.at[half_rows(xch, yb), :], cw_s.at[2], cw_r.at[2], ypeer))
    cw_f = go(rcopy(cw.at[half_rows(xch, yb), :], cw.at[half_rows(xch, yb), :], cw_s.at[3], cw_r.at[3], sib))
    tot = small_end(e1, q1, z1)
    mean1 = jnp.concatenate([tot[0:1], tot[1:2]], 1) * inv
    scale1 = lax.rsqrt(jnp.concatenate([tot[2:3], tot[3:4]], 1) * inv - mean1 * mean1 + norm_eps)
    gain2 = tot[4:5] * (1.0 / nseq)
    shift2 = tot[5:6] * (1.0 / nseq)
    gain1 = p1_ref[0:1, :]
    shift1 = p1_ref[1:2, :]

    def act_rows(i, _):
        at = pl.ds(pl.multiple_of(i * 32, 32), 32)
        v = (x_ref[at, :].astype(F32) - mean1) * scale1 * gain1 + shift1
        act[at, :] = gelu_of(v).astype(BF16)
        return 0

    lax.fori_loop(0, rows // 32, act_rows, 0)
    h_up = go(rcopy(act.at[pl.ds(0, 16), :], hin.at[1], hs_s.at[0], hs_r.at[0], before_id))
    h_dn = go(rcopy(act.at[pl.ds(rows - 16, 16), :], hin.at[0], hs_s.at[1], hs_r.at[1], after_id))
    send_w(order[1])
    pass_w(order[0])
    cw_y.wait_recv()
    cw_g = go(rcopy(cw.at[half_rows(xch, 1 - yb), :], cw.at[half_rows(xch, 1 - yb), :], cw_s.at[4], cw_r.at[4], sib))
    cw_sib.wait_recv()
    cw_f.wait_recv()
    cw_g.wait_recv()
    local[17].wait()
    start = line * rows - SHIFT + rows * nseq * 4
    first = (start % WINDOW_BINS) == 0
    last = ((start + rows) % WINDOW_BINS) == 0
    keep0 = jnp.where(first, 0.0, 1.0)
    keep2 = jnp.where(last, 0.0, 1.0)
    mine = pl.ds(16, rows)
    conv[...] = dot_nt(act[...], cw[:, 768:1536])
    tap0[mine, :] = dot_nt(act[...], cw[:, 0:768])
    tap2[mine, :] = dot_nt(act[...], cw[:, 1536:2304])
    h_up.wait_recv()
    h_dn.wait_recv()
    tap0[0:16, :] = dot_nt(hin[0], cw[:, 0:768]) * keep0
    tap2[pl.ds(rows + 16, 16), :] = dot_nt(hin[1], cw[:, 1536:2304]) * keep2
    step = DILATION_STEP
    full = conv[...] + tap0[pl.ds(16 - step, rows), :] + tap2[pl.ds(16 + step, rows), :]
    conv[...] = full
    m2[0:1, :] = jnp.sum(full, 0, keepdims=True)
    m2[1:2, :] = jnp.sum(full * full, 0, keepdims=True)
    e2 = small_start(1, m2, a2)
    for t in order[2:4]:
        send_w(t)
        send_w_sib(t)
    c_sib = []
    for j in range(7):
        c_sib.append(go(rcopy(cs_ref.at[1 - k, :, pl.ds(TILE * j, TILE)], cnt.at[j, my_bins, :], ct_s.at[j], ct_r.at[j], sib)))
    e2 = small_mid(1, e2, m2, a2, q2, z2)
    pass_w(order[1])
    send_w(order[4])
    tot2 = small_end(e2, q2, z2)
    mean2 = tot2[0:1] * inv
    scale2 = lax.rsqrt(tot2[1:2] * inv - mean2 * mean2 + norm_eps)

    def mix_rows(i, _):
        at = pl.ds(pl.multiple_of(i * 64, 64), 64)
        v = (conv[at, :] - mean2) * scale2 * gain2 + shift2
        a = gelu_of(v).astype(BF16)
        act2[at, :] = a
        o = (x_ref[at, :].astype(F32) + dot_nn(a, cw[:, 2304:])).astype(BF16)
        out_ref[at, :] = o
        orow[pl.ds(pl.multiple_of(rows * k + i * 64, 64), 64), :] = o
        return 0

    lax.fori_loop(0, rows // 64, mix_rows, 0)
    o_x = go(rcopy(out_ref, orow.at[my_bins, :], ox_s.at[0], ox_r.at[0], sib))
    for t in order[5:]:
        send_w(t)
    for t in order[4:]:
        send_w_sib(t)
    for t in order[2:4]:
        pass_w(t)
    o_x.wait_recv()
    both = 2 * rows
    ocol[...] = orow[...].T
    gacc[...] = jnp.zeros((both, 768), F32)
    bl[...] = jnp.zeros((16, TILE), F32)
    human = flag_ref[0]
    mouse = 1.0 - human

    def head_tile(j, w_at):
        bv = bv_ref[j]
        total = jnp.zeros((1, TILE), F32)
        for b in range(both // 128):
            at = pl.ds(128 * b, 128)
            z = dot_nn(orow[at, :], w_at[...]) + bv[0:1, :]
            g = (logit_slope(z, cnt[j, at, :].astype(F32)) * bv[1:2, :]).astype(BF16)
            gs[at, :] = g
            total = total + jnp.sum(g.astype(F32), 0, keepdims=True)
            gacc[at, :] = gacc[at, :] + dot_nt(g, w_at[...])
        for b in range(4):
            d = dot_nn(ocol[pl.ds(192 * b, 192), :], gs[...]).astype(BF16)
            for y in range(2):
                for xx in range(2):
                    f = xx + k * (y - xx)
                    g2 = y + k * (xx - y)
                    pbuf[j, f, g2, b % 2, b // 2] = d[96 * y + 48 * xx:96 * y + 48 * xx + 48, :]
        return total

    f_me = xb + k * (yb - xb)
    g_me = yb + k * (xb - yb)
    peer_a = (seq + k * (1 - 2 * yb), ch + (1 - k) * (2 - 4 * xb))
    peer_b = (seq + (1 - k) * (1 - 2 * yb), ch + k * (2 - 4 * xb))
    rs1 = {}


    for j in range(7):
        t_need = (j, 7 + j) if j < 3 else (j,)
        for t in order:
            if t not in wy and order.index(t) <= order.index(t_need[-1]) + 2:
                pass_w(t)
        for t in t_need:
            local[order.index(t)].wait()
            wsib[t].wait_recv()
            wy[t].wait_recv()
        local[10 + j].wait()
        c_sib[j].wait_recv()
        if j < 3:
            wsel[...] = (wh[j].astype(F32) * human + wm[j].astype(F32) * mouse).astype(BF16)
            total = head_tile(j, wsel)
            bl[8 + j:9 + j, :] = total * mouse
        else:
            total = head_tile(j, wh.at[j])
        bl[j:j + 1, :] = total * human
        rs1[j] = go(rcopy(pbuf.at[j, 1 - f_me], r1.at[j], rs_s.at[0, j], rs_r.at[0, j], peer_a))

    hp = flag_ref[1]
    mp = 1.0 - hp
    rs2, rs3, rs4, rs5 = {}, {}, {}, {}

    def adv1(j):
        rs1[j].wait_recv()
        own = pbuf[j, f_me].astype(F32)
        got = r1[j].astype(F32)
        b1[j] = (own * human + got * hp).astype(BF16)
        ts = [j]
        if j < 3:
            b1[7 + j] = (own * mouse + got * mp).astype(BF16)
            ts.append(7 + j)
        for t in ts:
            rs2[t] = go(rcopy(b1.at[t, 1 - g_me], r2.at[t], rs_s.at[1, t], rs_r.at[1, t], peer_b))

    def adv2(t):
        rs2[t].wait_recv()
        b2[t] = (b1[t, g_me].astype(F32) + r2[t].astype(F32)).astype(BF16)
        rs3[t] = go(rcopy(b2.at[t, 1 - z0], r3.at[t], rs_s.at[2, t], rs_r.at[2, t], zpeers[0]))

    def adv3(t):
        rs3[t].wait_recv()
        b3[t] = (b2[t, z0].astype(F32) + r3[t].astype(F32)).astype(BF16)
        rs4[t] = go(rcopy(b3.at[t, 1 - z1b], r4.at[t], rs_s.at[3, t], rs_r.at[3, t], zpeers[1]))

    def adv4(t):
        rs4[t].wait_recv()
        fin[t] = b3[t, z1b].astype(F32) + r4[t].astype(F32)
        rs5[t] = go(rcopy(fin.at[t, pl.ds(pl.multiple_of(24 - 24 * k, 8), 24), :], frecv.at[t], fx_s.at[t], fx_r.at[t], sib))

    g_x = go(rcopy(gacc.at[pl.ds(pl.multiple_of(rows * (1 - k), rows), rows), :], grecv, gh_s.at[0], gh_r.at[0], sib))
    bias_near = (near[1], near[3], near[5])
    bx = [go(rcopy(bl, bxy.at[i], bx_s.at[i], bx_r.at[i], bias_near[i])) for i in range(3)]
    g_x.wait_recv()

    def back_rows(i, carry):
        ga, sa = carry
        at = pl.ds(pl.multiple_of(i * 64, 64), 64)
        grad = gacc[pl.ds(pl.multiple_of(rows * k + i * 64, 64), 64), :] + grecv[at, :]
        grecv[at, :] = grad
        gb = grad.astype(BF16)
        gs2 = dot_nt(gb, cw[:, 2304:])
        nrm = (conv[at, :] - mean2) * scale2
        gp = gs2 * gelu_slope(nrm * gain2 + shift2)
        gpad[pl.ds(pl.multiple_of(16 + i * 64, 16), 64), :] = gp
        return ga + jnp.sum(gp * nrm, 0, keepdims=True), sa + jnp.sum(gp, 0, keepdims=True)

    zero_h = jnp.zeros((1, TILE), F32)
    ga2, sa2 = lax.fori_loop(0, rows // 64, back_rows, (zero_h, zero_h))
    m3[0:1, :] = ga2
    m3[1:2, :] = sa2
    e3 = small_start(2, m3, a3)

    def keep_piece(value, first_piece):
        low = value.astype(BF16)
        for c in range(4):
            for h in range(2):
                p = first_piece + h
                cgb[c % 2, c // 2, p // 4, (p // 2) % 2, p % 2] = low[96 * c:96 * c + 96, TILE * h:TILE * h + TILE]

    for j in range(2):
        adv1(j)
    e3 = small_mid(2, e3, m3, a3, q3, z3)
    keep_piece(dot_nn(act2[...].T, grecv[...].astype(BF16)), 6)
    adv1(2)
    adv1(3)
    tot3 = small_end(e3, q3, z3)
    s2_ref[...] = tot3
    gg2 = tot3[0:1]
    sg2 = tot3[1:2]

    def conv_rows(i, _):
        at = pl.ds(pl.multiple_of(i * 64, 64), 64)
        into = pl.ds(pl.multiple_of(16 + i * 64, 16), 64)
        nrm = (conv[at, :] - mean2) * scale2
        gc = (gain2 * scale2 * (gpad[into, :] - sg2 * inv - nrm * gg2 * inv)).astype(BF16)
        gsend[at, :] = gc
        gpad[into, :] = gc.astype(F32)
        return 0

    lax.fori_loop(0, rows // 64, conv_rows, 0)
    gh_up = go(rcopy(gsend.at[pl.ds(0, 16), :], ghalo.at[1], gh_s.at[1], gh_r.at[1], before_id))
    gh_dn = go(rcopy(gsend.at[pl.ds(rows - 16, 16), :], ghalo.at[0], gh_s.at[2], gh_r.at[2], after_id))
    adv1(4)
    adv1(5)
    adv2(0)
    acc1 = dot_nn(gsend[...], cw[:, 768:1536])
    keep_piece(dot_nn(gsend[...].T, act[...]), 2)
    gh_up.wait_recv()
    gh_dn.wait_recv()
    gpad[0:16, :] = ghalo[0].astype(F32) * keep0
    gpad[pl.ds(rows + 16, 16), :] = ghalo[1].astype(F32) * keep2
    gk[0] = gpad[pl.ds(16 + step, rows), :].astype(BF16)
    gk[1] = gpad[pl.ds(16 - step, rows), :].astype(BF16)
    g_x.wait_send()
    gacc[0:rows, :] = acc1 + dot_nn(gk[0], cw[:, 0:768]) + dot_nn(gk[1], cw[:, 1536:2304])

    def first_rows(i, carry):
        ga, sa = carry
        at = pl.ds(pl.multiple_of(i * 32, 32), 32)
        nrm = (x_ref[at, :].astype(F32) - mean1) * scale1
        gp = gacc[at, :] * gelu_slope(nrm * gain1 + shift1)
        gacc[at, :] = gp
        return ga + jnp.sum(gp * nrm, 0, keepdims=True), sa + jnp.sum(gp, 0, keepdims=True)

    zero_d = jnp.zeros((1, 768), F32)
    ga1, sa1 = lax.fori_loop(0, rows // 32, first_rows, (zero_d, zero_d))
    m4[0:1, :] = ga1[:, :TILE]
    m4[1:2, :] = ga1[:, TILE:]
    m4[2:3, :] = sa1[:, :TILE]
    m4[3:4, :] = sa1[:, TILE:]
    e4 = small_start(3, m4, a4)
    keep_piece(dot_nn(gk[0].T, act[...]), 0)
    keep_piece(dot_nn(gk[1].T, act[...]), 4)
    c1 = go(rcopy(cgb.at[1 - k], crc, cg_s.at[0], cg_r.at[0], sib))
    e4 = small_mid(3, e4, m4, a4, q4, z4)
    adv1(6)

    def add_into(dst, one, two):
        dst[...] = (one.astype(F32) + two.astype(F32)).astype(BF16)

    c1.wait_recv()
    add_into(csc, cgb[k], crc[...])
    c2 = go(rcopy(csc.at[1 - xb], crx, cg_s.at[1], cg_r.at[1], xpeer))
    for t in (7, 1, 8, 2):
        adv2(t)
    tot4 = small_end(e4, q4, z4)
    s1_ref[...] = tot4
    gg1 = jnp.concatenate([tot4[0:1], tot4[1:2]], 1)
    sg1 = jnp.concatenate([tot4[2:3], tot4[3:4]], 1)

    def last_rows(i, _):
        at = pl.ds(pl.multiple_of(i * 32, 32), 32)
        nrm = (x_ref[at, :].astype(F32) - mean1) * scale1
        ig_ref[at, :] = grecv[at, :] + gain1 * scale1 * (gacc[at, :] - sg1 * inv - nrm * gg1 * inv)
        return 0

    lax.fori_loop(0, rows // 32, last_rows, 0)
    for c in bx:
        c.wait_recv()
    bs[...] = tree([bl[...], bxy[0], bxy[1], bxy[2]])
    bz_c = [go(rcopy(bs, bz.at[i], bx_s.at[3 + i], bx_r.at[3 + i], zpeers[i])) for i in range(3)]
    for t in (9, 3):
        adv2(t)
    for t in (0, 7, 1):
        adv3(t)
    c2.wait_recv()
    add_into(csx, csc[xb], crx[...])
    c3 = go(rcopy(csx.at[1 - yb], cry, cg_s.at[2], cg_r.at[2], ypeer))
    for t in (4, 5, 6):
        adv2(t)
    for t in (8, 2, 9):
        adv3(t)
    for t in (0, 7, 1):
        adv4(t)
    c3.wait_recv()
    add_into(csy, csx[yb], cry[...])
    c4 = go(rcopy(csy.at[1 - z0], crz, cg_s.at[3], cg_r.at[3], zpeers[0]))
    for t in (3, 4):
        adv3(t)
    c4.wait_recv()
    add_into(csz, csy[z0], crz[...])
    c5 = go(rcopy(csz.at[1 - z1b], crw, cg_s.at[4], cg_r.at[4], zpeers[1]))
    for t in (8, 2, 9):
        adv4(t)
    c5.wait_recv()
    cao[yb, z0, z1b] = (csz[z1b].astype(F32) + crw[...].astype(F32)).astype(BF16)
    here = cao.at[yb, z0, z1b]
    c6 = go(rcopy(here, here, cg_s.at[5], cg_r.at[5], zpeers[1]))
    for t in (5, 6):
        adv3(t)
    c6.wait_recv()
    here = cao.at[yb, z0]
    c7 = go(rcopy(here, here, cg_s.at[6], cg_r.at[6], zpeers[0]))
    for t in (3, 4):
        adv4(t)
    c7.wait_recv()
    here = cao.at[yb]
    c8 = go(rcopy(here, here, cg_s.at[7], cg_r.at[7], ypeer))
    for t in (5, 6):
        adv4(t)
    for c in bz_c:
        c.wait_recv()
    bg_ref[k] = tree([bs[...], bz[0], bz[1], bz[2]])
    bs2 = go(rcopy(bg_ref.at[k], bg_ref.at[k], bx_s.at[6], bx_r.at[6], sib))
    mine24 = pl.ds(pl.multiple_of(24 * k, 8), 24)
    for t in (0, 7, 1, 8, 2, 9, 3, 4, 5, 6):
        rs5[t].wait_recv()
        if t < 7:
            oh_ref[:, human_cols(t, k)] = fin[t, mine24, :]
            oh_ref[:, human_cols(t, 1 - k)] = frecv[t]
        else:
            wide = TILE if t < 9 else 128
            om_ref[:, mouse_cols(t - 7, k)] = fin[t, mine24, 0:wide]
            om_ref[:, mouse_cols(t - 7, 1 - k)] = frecv[t, :, 0:wide]
    c8.wait_recv()
    cg_ref[...] = cao[...].astype(F32)
    bs2.wait_recv()
    for c in sent:
        if c is not g_x:
            c.wait_send()


def fused_on_device(
    inputs, gain_one, shift_one, conv_weight, gain_two, shift_two, mix_weight, head_weight, head_bias, species, counts
):
    nseq = lax.axis_size("seq")
    seq = lax.axis_index("seq")
    ch = lax.axis_index("ch")
    k = ch % 2
    rows, width = inputs.shape
    bins = rows * 4 * nseq
    tracks = head_weight.shape[1]
    hid = 96 * 4

    def is_human(s, c):
        w = window_lookup(s * rows * 4 + c * rows, bins)
        ids = jnp.arange(species.shape[0], dtype=jnp.int32)
        return jnp.sum(jnp.where(ids == w, species, 0)) == 0

    human = is_human(seq, ch)
    peer_seq = seq + k * (1 - 2 * (seq % 2))
    peer_ch = ch + (1 - k) * (2 - 4 * (ch // 2))
    flags = jnp.stack([human, is_human(peer_seq, peer_ch)]).astype(F32)
    cw_own = jnp.concatenate([conv_weight.transpose(2, 0, 1).reshape(96, TAPS * width), mix_weight], 1)
    zero = jnp.zeros((2, hid), F32)
    g2 = lax.dynamic_update_slice(zero, jnp.stack([gain_two, shift_two]), (0, 96 * ch))
    p1 = jnp.stack([gain_one, shift_one])
    edge = HUMAN // 128 * 128
    skip = HUMAN - edge
    wm = jnp.pad(head_weight[:, edge:], ((0, 0), (0, 1792 - (tracks - edge))))

    def human_counts(unused):
        c = jnp.pad(counts.astype(BF16), ((0, 0), (0, 5376 - HUMAN)))
        return jnp.stack([c[:, :2688], c[:, 2688:]])

    def mouse_counts(unused):
        c = jnp.pad(counts[:, :MOUSE].astype(BF16), ((0, 0), (skip, 1792 - skip - MOUSE)))
        more = ((0, 0), (0, 2688 - 896))
        return jnp.stack([jnp.pad(c[:, :896], more), jnp.pad(c[:, 896:], more)])

    cs = lax.cond(human, human_counts, mouse_counts, 0)
    hb = jnp.pad(head_bias[:HUMAN], (0, 5376 - HUMAN)).reshape(2, 2688)
    hv = jnp.pad(jnp.ones((HUMAN,), F32), (0, 5376 - HUMAN)).reshape(2, 2688)
    mb = jnp.pad(head_bias[HUMAN:], (skip, 1792 - skip - MOUSE)).reshape(2, 896)
    mv = jnp.pad(jnp.ones((MOUSE,), F32), (skip, 1792 - skip - MOUSE)).reshape(2, 896)
    more = ((0, 0), (0, 2688 - 896))
    bv = jnp.where(human, jnp.stack([hb, hv]), jnp.stack([jnp.pad(mb, more), jnp.pad(mv, more)]))
    bv = jnp.where(k == 0, bv[:, 0], bv[:, 1]).reshape(2, 7, TILE).transpose(1, 0, 2)

    V = pltpu.VMEM
    D = pltpu.SemaphoreType.DMA
    vm = pl.BlockSpec(memory_space=pltpu.VMEM)
    anywhere = pl.BlockSpec(memory_space=pl.ANY)
    small = [(8, TILE), (2, TILE), (2, TILE), (4, TILE)]
    scratch = [
        V((rows, width), BF16), V((2, 16, width), BF16), V((hid, 4 * width), BF16), V((rows, hid), F32),
        V((rows + 32, hid), F32), V((rows + 32, hid), F32),
        V((7, 768, TILE), BF16), V((3, 768, TILE), BF16), V((768, TILE), BF16), V((7, 2 * rows, TILE), BF16),
        V((2 * rows, width), BF16), V((width, 2 * rows), BF16), V((2 * rows, TILE), BF16),
        V((2 * rows, width), F32), V((rows, width), F32),
        V((7, 2, 2, 2, 2, 48, TILE), BF16), V((7, 2, 2, 2, 48, TILE), BF16), V((10, 2, 2, 2, 48, TILE), BF16),
        V((10, 2, 2, 48, TILE), BF16), V((10, 2, 2, 48, TILE), BF16),
        V((10, 2, 48, TILE), BF16), V((10, 2, 48, TILE), BF16), V((10, 48, TILE), BF16),
        V((10, 48, TILE), F32), V((10, 24, TILE), F32),
        *[V(s, F32) for s in small],
        *[V((7, *s), F32) for s in small],
        *[V((3, *s), F32) for s in small],
        *[V(s, F32) for s in small],
        V((16, TILE), F32), V((3, 16, TILE), F32), V((16, TILE), F32), V((3, 16, TILE), F32),
        V((rows + 32, hid), F32), V((rows, hid), BF16), V((2, 16, hid), BF16), V((2, rows, hid), BF16), V((rows, hid), BF16),
        V((2, 2, 2, 2, 2, 96, TILE), BF16), V((2, 2, 2, 2, 96, TILE), BF16), V((2, 2, 2, 2, 96, TILE), BF16),
        V((2, 2, 2, 96, TILE), BF16), V((2, 2, 2, 96, TILE), BF16),
        V((2, 2, 96, TILE), BF16), V((2, 2, 96, TILE), BF16),
        V((2, 96, TILE), BF16), V((2, 96, TILE), BF16), V((96, TILE), BF16), V((2, 2, 2, 96, TILE), BF16),
        D((4, 10)), D((4, 10)), D((2,)), D((2,)), D((6,)), D((6,)), D((10,)), D((10,)), D((10,)), D((10,)), D((10,)),
        D((10,)), D((10,)), D((7,)), D((7,)), D((7,)),
        D((1,)), D((1,)), D((4, 10)), D((4, 10)), D((10,)), D((10,)), D((7,)), D((7,)), D((3,)), D((3,)), D((8,)), D((8,)),
    ]
    S = jax.ShapeDtypeStruct
    outs = pl.pallas_call(
        step_kernel,
        out_shape=[
            S((rows, width), BF16), S((rows, width), F32), S((4, TILE), F32), S((2, hid), F32),
            S((2, 2, 2, 96, TILE), F32), S((24, 5376), F32), S((24, 1792), F32), S((2, 16, TILE), F32),
        ],
        in_specs=[vm, vm, vm, vm, anywhere, anywhere, anywhere, vm, pl.BlockSpec(memory_space=pltpu.SMEM)],
        out_specs=[vm] * 8,
        scratch_shapes=scratch,
        compiler_params=pltpu.CompilerParams(collective_id=0, has_side_effects=True, vmem_limit_bytes=64 * 1024 * 1024 - 128 * 1024),
        name="step",
    )(inputs, p1, g2, cw_own, head_weight, wm, cs, bv, flags)
    out, ig, s1, s2, cg, oh, om, bg = outs
    cg = cg.reshape(4, 2, 96, TILE)
    conv_grad = cg[:3].transpose(0, 1, 3, 2).reshape(TAPS, width, 96)
    mix_grad = cg[3].transpose(1, 0, 2).reshape(96, width)
    s2 = lax.dynamic_slice(s2, (0, 96 * ch), (2, 96))
    head_grad = jnp.concatenate([oh[:, :HUMAN], om[:, skip:skip + MOUSE]], 1)
    bias_h = bg[:, :7].reshape(2, 2688).reshape(-1)[:HUMAN]
    bias_m = bg[:, 8:11].reshape(2, 3 * TILE)[:, :896].reshape(-1)[skip:skip + MOUSE]
    return (
        out, ig, s1[:2].reshape(-1), s1[2:].reshape(-1), conv_grad, s2[0], s2[1], mix_grad, head_grad,
        jnp.concatenate([bias_h, bias_m]),
    )


def solution(mesh):
    in_specs = (
        P(("seq", "ch"), None),
        P(),
        P(),
        P(None, None, "ch"),
        P("ch"),
        P("ch"),
        P("ch", None),
        P("ch", None),
        P(),
        P(),
        P(("seq", "ch"), None),
    )
    out_specs = (
        P(("seq", "ch"), None),
        P(("seq", "ch"), None),
        P(),
        P(),
        P(None, None, "ch"),
        P("ch"),
        P("ch"),
        P("ch", None),
        P(("seq", "ch"), None),
        P(),
    )
    fits = mesh.shape["seq"] == 8 and mesh.shape["ch"] == 4
    body = fused_on_device if fits else on_device
    return jax.shard_map(
        body, mesh=mesh, in_specs=in_specs, out_specs=out_specs, check_vma=False
    )
```
